32 devices in a mesh: dom: 8 (over z, y), rep: 4 (over x, core).
Axes of the slice: x: 2, y: 2, z: 4, core: 2. Of those that a mesh axis runs over, the one named last changes fastest.
Arguments:
- ns_shape: bfloat16 [64, 256], replicated, may hold values from -0.75 to 0.75
- nm_shape: bfloat16 [64, 256], replicated, may hold values from -0.75 to 0.75
- sec_disp: bfloat16 [64, 262144], P(None, ('dom', 'rep')), may hold values from -6 to 6
- mst_disp: bfloat16 [64, 262144], P(None, ('dom', 'rep')), may hold values from -6 to 6
- gap_offset: float32 [262144], P(('dom', 'rep')), may hold values from -6 to 6
- quad_weight: float32 [256], replicated, may hold values from 0.25 to 4
- jacobian: float32 [262144], P(('dom', 'rep')), may hold values from 0.0005 to 0.005
- segment_slot: int32 [262144], P(('dom', 'rep')), may hold values from 0 to 1279, as said below
- face_id: int32 [262144], P(('dom', 'rep')), may hold values from 0 to 1073741823
- search_rank: int32 [262144], P(('dom', 'rep')), may hold values from 0 to 3
- live_rows: int32 [32], P(('dom', 'rep')), may hold values from 1024 to 8192, as said below
Outputs:
- contact_force: bfloat16 [64, 262144], P(None, ('dom', 'rep'))
- seg_pen: float32 [8192], P('dom')
- seg_face: int32 [8192], P('dom')
- seg_gap: float32 [8192], P('dom')
- mean_gap: float32 [], replicated
The draws below stay inside these ranges and needn't reach their ends.
Inputs may be any that keep to these rules, and one draw needn't show every extreme that they name: `segment_slot`: A row's segment is (1024 times the dom index of its device plus its slot) modulo 8192; slots of 1024 or more reach the next dom index's first 256 segments. `live_rows`: entry b counts the live rows of the device with flat index b (dom-major); they are that device's first rows, the rest are padding; some device is full in every draw.
All inputs are finite; a program needn't handle non-finite values.
Results may differ from the reference program's by a relative error of at most 0.0055.
Values sent between devices are 32-bit elements; how exact they have to be, the bound alone decides.
No kernel may reach another device: no remote copies, remote signals or barrier semaphores. Data moves between devices by JAX's collectives and lax.ppermute only.
A program may use at most 64 MiB of HBM per device.

```python
import math
import jax
import jax.numpy as jnp
from jax import lax

P_SIZE = 256
K = 64
ROWS_DEV = 8192
SEG_DEV = 1024
SPILL = 256
SEGS = 8192
ROWS = 262144
N_REP = 4
DEVICES = 32


def draw_live_rows(key, part):
    first_key = jax.random.fold_in(key, 11)
    second_key = jax.random.fold_in(key, 23)
    counts = jax.random.randint(first_key, (DEVICES,), ROWS_DEV // 8, ROWS_DEV + 1, dtype=jnp.int32)
    full_device = jax.random.randint(second_key, (), 0, DEVICES, dtype=jnp.int32)
    return jnp.where(jnp.arange(DEVICES, dtype=jnp.int32) == full_device, ROWS_DEV, counts).astype(jnp.int32)


def draw_segment_slot(key, part):
    window_len = SEG_DEV + SPILL
    dom_count = DEVICES // N_REP
    vacant = jax.random.randint(jax.random.fold_in(key, 31), (SEGS,), 0, 8, dtype=jnp.int32) == 0
    forced = jax.random.randint(jax.random.fold_in(key, 37), (), 0, SEGS, dtype=jnp.int32)
    vacant = vacant | (jnp.arange(SEGS, dtype=jnp.int32) == forced)
    dom_ids = jnp.arange(dom_count, dtype=jnp.int32)
    window_ids = ((dom_ids[:, None] * SEG_DEV + jnp.arange(window_len, dtype=jnp.int32)[None, :]) % SEGS).astype(jnp.int32)
    blocked = vacant[window_ids].astype(jnp.int32)
    order = jnp.argsort(blocked, axis=1, stable=True).astype(jnp.int32)
    allowed = jnp.maximum(window_len - jnp.sum(blocked, axis=1), 1).astype(jnp.int32)
    row_dom = (jnp.arange(ROWS, dtype=jnp.int32) // (ROWS_DEV * N_REP)).astype(jnp.int32)
    raw_pick = jax.random.randint(jax.random.fold_in(key, 41), (ROWS,), 0, 1 << 24, dtype=jnp.int32)
    pick = (raw_pick % allowed[row_dom]).astype(jnp.int32)
    return order[row_dom, pick].astype(jnp.int32)


def set_ends(drawn, own_key, least, top_value):
    longest = drawn.shape.index(max(drawn.shape))
    spots = []
    for shift in (0, 1):
        where = [jax.random.randint(jax.random.fold_in(own_key, axis), (), 0, length) for axis, length in enumerate(drawn.shape)]
        where[longest] = (where[longest] + shift) % drawn.shape[longest]
        spots.append(tuple(where))
    return drawn.at[spots[0]].set(least).at[spots[1]].set(top_value)


def levels(stream_key, extent, cuts, least, high):
    level, own = 1.0, jax.random.fold_in(stream_key, 6)
    for dim, shards_of in cuts:
        steps = jnp.exp(jax.random.uniform(jax.random.fold_in(own, dim), (shards_of,), jnp.float32, least / len(cuts), high / len(cuts)))
        level = level * jnp.repeat(steps, extent[dim] // shards_of).reshape([-1 if axis == dim else 1 for axis in range(len(extent))])
    return level


def centred(key, extent, scale, most, pieces=(), held_as=jnp.bfloat16):
    result = scale * jax.random.normal(key, extent, jnp.float32)
    if pieces:
        result = result * levels(key, extent, pieces, -0.22, 0.18)
    return jnp.clip(result, -most, most).astype(held_as)


def setup_inputs(seed: int = 0) -> dict:
    key_of = jax.random.split(jax.random.key(seed), 12)
    return {
        "ns_shape": centred(key_of[0], (K, P_SIZE), K ** -0.5, 0.75),
        "nm_shape": centred(key_of[1], (K, P_SIZE), K ** -0.5, 0.75),
        "sec_disp": centred(key_of[2], (K, ROWS), 1.0, 6.0, ((1, 32),)),
        "mst_disp": centred(key_of[3], (K, ROWS), 1.0, 6.0, ((1, 32),)),
        "gap_offset": centred(key_of[4], (ROWS,), 1.0, 6.0, ((0, 32),), jnp.float32),
        "quad_weight": jnp.clip(jnp.exp(jax.random.uniform(key_of[5], (P_SIZE,), jnp.float32, math.log(0.25), math.log(4.0))), 0.25, 4.0),
        "jacobian": jnp.clip(jnp.exp(math.log(0.005) - 2.30258502 * jax.random.uniform(key_of[6], (ROWS,), jnp.float32) ** levels(key_of[6], (ROWS,), ((0, 32),), -0.2, 0.2)), 0.0005, 0.005),
        "segment_slot": draw_segment_slot(jax.random.fold_in(key_of[11], 71), 0),
        "face_id": set_ends(jax.random.randint(key_of[8], (ROWS,), 0, 1073741824), jax.random.fold_in(key_of[8], 1), 0, 1073741823).astype(jnp.int32),
        "search_rank": set_ends(jax.random.randint(key_of[9], (ROWS,), 0, 4), jax.random.fold_in(key_of[9], 1), 0, 3).astype(jnp.int32),
        "live_rows": draw_live_rows(jax.random.fold_in(key_of[11], 71), 0),
    }


PENALTY = 400.0
LOWEST_FILL = -1.0e30
FACE_LIMIT = 1073741824


def project(shape_table, displace):
    return lax.dot_general(shape_table, displace, (((0,), (0,)), ((), ())), preferred_element_type=jnp.float32)


def window_stats(gap_field, jac_row, weights, slots, faces, ranks, live, window_len):
    row_pen = jnp.max(-gap_field, axis=0)
    row_gap = jac_row * jnp.dot(weights, gap_field, precision=lax.Precision.HIGHEST)
    row_area = jac_row * jnp.sum(weights)
    penalty_max = jnp.maximum(jax.ops.segment_max(jnp.where(live, row_pen, LOWEST_FILL), slots, num_segments=window_len), LOWEST_FILL)
    best_rank = jnp.maximum(jax.ops.segment_max(jnp.where(live, ranks, -1), slots, num_segments=window_len), -1).astype(jnp.int32)
    chosen = jnp.where(live & (ranks == best_rank[slots]), faces, FACE_LIMIT).astype(jnp.int32)
    lowest_face = jnp.minimum(jax.ops.segment_min(chosen, slots, num_segments=window_len), FACE_LIMIT).astype(jnp.int32)
    gap_sum = jax.ops.segment_sum(jnp.where(live, row_gap, 0.0), slots, num_segments=window_len)
    area_sum = jax.ops.segment_sum(jnp.where(live, row_area, 0.0), slots, num_segments=window_len)
    return penalty_max, best_rank, lowest_face, gap_sum, area_sum


def reference(ns_shape, nm_shape, sec_disp, mst_disp, gap_offset, quad_weight, jacobian, segment_slot, face_id, search_rank, live_rows):
    row_count = ROWS_DEV
    window_len = SEG_DEV + SPILL

    def blocks(values):
        return values.reshape(DEVICES, row_count)

    sec_blocks = sec_disp.reshape(K, DEVICES, row_count).transpose(1, 0, 2)
    mst_blocks = mst_disp.reshape(K, DEVICES, row_count).transpose(1, 0, 2)

    def one_block(block):
        sec_part, mst_part, offset, jac_row, slots, faces, ranks, live_count = block
        gap_field = project(ns_shape, sec_part) - project(nm_shape, mst_part) + offset[None, :]
        live = jnp.arange(row_count, dtype=jnp.int32) < live_count
        load = jnp.where(live[None, :], quad_weight[:, None] * jac_row[None, :] * PENALTY * jnp.maximum(-gap_field, 0.0), 0.0).astype(jnp.bfloat16)
        force = jnp.dot(ns_shape, load, preferred_element_type=jnp.float32).astype(jnp.bfloat16)
        stats = window_stats(gap_field, jac_row, quad_weight, slots, faces, ranks, live, window_len)
        return (force,) + stats

    outputs = lax.map(one_block, (sec_blocks, mst_blocks, blocks(gap_offset), blocks(jacobian), blocks(segment_slot), blocks(face_id), blocks(search_rank), live_rows))
    force_blocks, penalty_max, best_rank, lowest_face, gap_sum, area_sum = outputs
    contact_force = force_blocks.transpose(1, 0, 2).reshape(K, DEVICES * row_count)
    dom_index = (jnp.arange(DEVICES, dtype=jnp.int32) // N_REP).astype(jnp.int32)
    seg_ids = ((dom_index[:, None] * SEG_DEV + jnp.arange(window_len, dtype=jnp.int32)[None, :]) % SEGS).astype(jnp.int32).reshape(-1)
    seg_max = jnp.maximum(jax.ops.segment_max(penalty_max.reshape(-1), seg_ids, num_segments=SEGS), LOWEST_FILL)
    seg_rank = jnp.maximum(jax.ops.segment_max(best_rank.reshape(-1), seg_ids, num_segments=SEGS), -1).astype(jnp.int32)
    chosen = jnp.where(best_rank.reshape(-1) == seg_rank[seg_ids], lowest_face.reshape(-1), FACE_LIMIT).astype(jnp.int32)
    seg_low = jnp.minimum(jax.ops.segment_min(chosen, seg_ids, num_segments=SEGS), FACE_LIMIT).astype(jnp.int32)
    seg_pen = jnp.where(seg_rank < 0, jnp.float32(0.0), seg_max)
    seg_face = jnp.where(seg_rank < 0, -1, seg_low).astype(jnp.int32)
    seg_gap = jax.ops.segment_sum(gap_sum.reshape(-1), seg_ids, num_segments=SEGS)
    mean_gap = jnp.sum(gap_sum) / jnp.sum(area_sum)
    return contact_force, seg_pen, seg_face, seg_gap, mean_gap
```

```python
import functools

import jax
import jax.numpy as jnp
from jax import lax
from jax.experimental import pallas as pl
from jax.experimental.pallas import tpu as pltpu
from jax.sharding import PartitionSpec as P

SEG_DEV = 1024
SPILL = 256


PENALTY = 400.0
LOWEST_FILL = -1e30
FACE_LIMIT = 1073741824
LANES = 128
GROUP = 16
NO_KEY = -(2**31)


def pieces_of(value, count):
    parts = []
    for _ in range(count):
        part = value.astype(jnp.bfloat16).astype(jnp.float32)
        parts.append(part)
        value = value - part
    return parts


def local_kernel(
    live_ref,
    ns_ref,
    nm_ref,
    weight_ref,
    sec_ref,
    mst_ref,
    offset_ref,
    jac_ref,
    slot_ref,
    face_ref,
    rank_ref,
    force_ref,
    table_ref,
    table_w,
    wide_weight,
):
    step = pl.program_id(0)
    points = ns_ref.shape[1]
    nodes = ns_ref.shape[0]
    rows = sec_ref.shape[1]
    blocks = rows // LANES
    bf16, f32, i32 = jnp.bfloat16, jnp.float32, jnp.int32

    @pl.when(step == 0)
    def _():
        weight = weight_ref[...]
        ns32, nm32 = ns_ref[...].astype(f32), nm_ref[...].astype(f32)
        wide_weight[...] = jnp.transpose(jnp.broadcast_to(weight, (LANES, points)))
        both = jnp.concatenate([ns32, -nm32], axis=0)
        tops = jnp.sum(both * weight, axis=1, keepdims=True)
        ones_at = lax.broadcasted_iota(i32, (GROUP, points), 0) < 3
        total = jnp.sum(weight, axis=1, keepdims=True)
        tails = jnp.broadcast_to(total, (GROUP, LANES))
        tail_parts = pieces_of(tails, 3)
        top_parts = pieces_of(jnp.broadcast_to(tops, (2 * nodes, LANES)), 3)
        lane = lax.broadcasted_iota(i32, (2 * nodes, LANES), 1)
        head = jnp.where(lane == 0, top_parts[0], jnp.where(lane == 1, top_parts[1], jnp.where(lane == 2, top_parts[2], 0.0)))
        lane = lax.broadcasted_iota(i32, (GROUP, LANES), 1)
        sub = lax.broadcasted_iota(i32, (GROUP, LANES), 0)
        foot = jnp.where(lane == 0, tail_parts[0], jnp.where(lane == 1, tail_parts[1], jnp.where(lane == 2, tail_parts[2], 0.0)))
        foot = jnp.where(sub < 3, foot, 0.0)
        left = jnp.concatenate([both, ones_at.astype(f32)], axis=0)
        right = jnp.concatenate([head, foot], axis=0)
        table_w[0:points, :] = jnp.transpose(left).astype(bf16)
        table_w[points:, :] = jnp.transpose(right).astype(bf16)[0:GROUP, :]
        table_ref[0:GROUP, :] = jnp.full((GROUP, LANES), LOWEST_FILL, f32)
        table_ref[GROUP:, :] = jnp.zeros((table_ref.shape[0] - GROUP, LANES), f32)

    live_count = live_ref[0]
    row_ids = (
        step * rows
        + LANES * lax.broadcasted_iota(i32, (blocks, LANES), 0)
        + lax.broadcasted_iota(i32, (blocks, LANES), 1)
    )
    live = row_ids < live_count
    jac = jac_ref[...]

    def as_row(value):
        return jnp.concatenate([value[b : b + 1, :] for b in range(blocks)], axis=1)

    def as_block(value):
        return jnp.concatenate([value[:, LANES * b : LANES * (b + 1)] for b in range(blocks)], axis=0)

    off = pieces_of(offset_ref[...], 3)
    sub = lax.broadcasted_iota(i32, (GROUP, rows), 0)
    off_rows = jnp.where(
        sub == 0, as_row(off[0]), jnp.where(sub == 1, as_row(off[1]), jnp.where(sub == 2, as_row(off[2]), 0.0))
    ).astype(bf16)
    stacked = jnp.concatenate([sec_ref[...], mst_ref[...], off_rows], axis=0)
    gaps = jnp.dot(table_w[...], stacked, preferred_element_type=f32)
    field = gaps[0:points, :]
    pen = as_block(-jnp.min(field, axis=0, keepdims=True))
    weighted = as_block(gaps[points : points + 1, :] + gaps[points + 1 : points + 2, :] + gaps[points + 2 : points + 3, :])

    weights = wide_weight[...]
    scale = jnp.where(live, jac * -PENALTY, 0.0)
    loads = jnp.concatenate(
        [
            (jnp.minimum(field[:, LANES * b : LANES * (b + 1)], 0.0) * weights).astype(bf16)
            for b in range(blocks)
        ],
        axis=1,
    )
    force = jnp.dot(ns_ref[...], loads, preferred_element_type=f32)
    force_ref[...] = (force * as_row(scale)).astype(bf16)

    row_gap = jnp.where(live, jac * weighted, 0.0)
    row_area = jnp.where(live, jac * jnp.sum(weight_ref[...], axis=1, keepdims=True), 0.0)
    table_ref[5 * GROUP : 5 * GROUP + blocks, :] += row_gap
    table_ref[5 * GROUP + 8 : 5 * GROUP + 8 + blocks, :] += row_area

    slot = jnp.where(live, slot_ref[...], (GROUP - 1) * LANES)
    key = ((rank_ref[...] - 2) << 30) + (FACE_LIMIT - 1 - face_ref[...])
    gap_parts = pieces_of(row_gap, 3)
    slot_t, pen_t, key_t = jnp.transpose(slot), jnp.transpose(pen), jnp.transpose(key)
    sub = lax.broadcasted_iota(i32, (LANES, LANES), 0)
    lane = lax.broadcasted_iota(i32, (LANES, LANES), 1)
    group_id = lax.broadcasted_iota(i32, (GROUP, LANES), 0)
    for b in range(blocks):
        slot_col = jnp.broadcast_to(slot_t[:, b : b + 1], (LANES, LANES))
        slot_row = slot[b : b + 1, :]
        same = slot_col == slot_row
        top_pen = jnp.max(jnp.where(same, pen_t[:, b : b + 1], LOWEST_FILL), axis=0, keepdims=True)
        top_key = jnp.max(jnp.where(same, key_t[:, b : b + 1], NO_KEY), axis=0, keepdims=True)
        last = jnp.max(jnp.where(same, sub, -1), axis=0, keepdims=True)
        speaks = last == lax.broadcasted_iota(i32, (1, LANES), 1)
        home = (slot_row >> 7) == group_id
        spoken = home & speaks
        one_hot = jnp.where((slot_col & (LANES - 1)) == lane, 1.0, 0.0).astype(bf16)
        values = pieces_of(top_pen, 3) + [
            (top_key & 255).astype(f32),
            ((top_key >> 8) & 255).astype(f32),
            ((top_key >> 16) & 255).astype(f32),
            (top_key >> 24).astype(f32),
        ]
        picks = [jnp.where(spoken, value, 0.0) for value in values]
        picks.append(jnp.where(spoken, 1.0, 0.0))
        picks += [jnp.where(home, part[b : b + 1, :], 0.0) for part in gap_parts]
        left = jnp.concatenate(picks, axis=0).astype(bf16)
        out = jnp.dot(left, one_hot, preferred_element_type=f32)
        part = [out[GROUP * i : GROUP * (i + 1), :] for i in range(11)]
        there = part[7] > 0.5
        fresh_pen = jnp.where(there, (part[0] + part[1]) + part[2], LOWEST_FILL)
        fresh_high = part[6] * 256.0 + part[5]
        fresh_low = part[4] * 256.0 + part[3]
        old_pen = table_ref[0:GROUP, :]
        old_high = table_ref[GROUP : 2 * GROUP, :]
        old_low = table_ref[2 * GROUP : 3 * GROUP, :]
        fresh_wins = there & (
            (old_pen == LOWEST_FILL)
            | (fresh_high > old_high)
            | ((fresh_high == old_high) & (fresh_low > old_low))
        )
        table_ref[0:GROUP, :] = jnp.maximum(old_pen, fresh_pen)
        table_ref[GROUP : 2 * GROUP, :] = jnp.where(fresh_wins, fresh_high, old_high)
        table_ref[2 * GROUP : 3 * GROUP, :] = jnp.where(fresh_wins, fresh_low, old_low)
        table_ref[3 * GROUP : 4 * GROUP, :] += (part[8] + part[9]) + part[10]


def local_step(ns, nm, sec, mst, offset, weight, jac, slot, face, rank, live):
    nodes, points = ns.shape
    row_count = sec.shape[1]
    rows = min(row_count, 1024)
    folded = lambda value: value.reshape(row_count // LANES, LANES)
    whole = lambda shape: pl.BlockSpec(shape, lambda i: (0, 0))
    wide = pl.BlockSpec((nodes, rows), lambda i: (0, i))
    tall = pl.BlockSpec((rows // LANES, LANES), lambda i: (i, 0))
    return pl.pallas_call(
        local_kernel,
        grid=(row_count // rows,),
        in_specs=[
            pl.BlockSpec(memory_space=pltpu.SMEM),
            whole((nodes, points)),
            whole((nodes, points)),
            whole((1, points)),
            wide,
            wide,
            tall,
            tall,
            tall,
            tall,
            tall,
        ],
        out_specs=[wide, whole((6 * GROUP, LANES))],
        out_shape=[
            jax.ShapeDtypeStruct((nodes, row_count), jnp.bfloat16),
            jax.ShapeDtypeStruct((6 * GROUP, LANES), jnp.float32),
        ],
        scratch_shapes=[
            pltpu.VMEM((points + GROUP, 2 * nodes + GROUP), jnp.bfloat16),
            pltpu.VMEM((points, LANES), jnp.float32),
        ],
    )(
        live,
        ns,
        nm,
        weight.reshape(1, points),
        sec,
        mst,
        folded(offset),
        folded(jac),
        folded(slot),
        folded(face),
        folded(rank),
    )


def sent(value, dom_by, rep_by):
    doms, reps = lax.axis_size("dom"), lax.axis_size("rep")
    pairs = [
        (d * reps + r, (d + dom_by) % doms * reps + (r + rep_by) % reps)
        for d in range(doms)
        for r in range(reps)
    ]
    return lax.ppermute(value, ("dom", "rep"), pairs)


def merge(first, second):
    wins = (second[1] > first[1]) | ((second[1] == first[1]) & (second[2] > first[2]))
    wins = (second[0] > LOWEST_FILL) & (wins | (first[0] <= LOWEST_FILL))
    return (
        jnp.maximum(first[0], second[0]),
        jnp.where(wins, second[1], first[1]),
        jnp.where(wins, second[2], first[2]),
        first[3] + second[3],
    )


def shards(ns, nm, sec, mst, offset, weight, jac, slot, face, rank, live):
    doms, reps = lax.axis_size("dom"), lax.axis_size("rep")
    own_rows, spill_rows = SEG_DEV // LANES, SPILL // LANES
    force, table = local_step(ns, nm, sec, mst, offset, weight, jac, slot, face, rank, live)
    planes = [table[GROUP * i : GROUP * (i + 1)] for i in range(4)]
    totals = jnp.stack([jnp.sum(table[5 * GROUP : 5 * GROUP + 8]), jnp.sum(table[5 * GROUP + 8 :])])
    totals = jnp.pad(totals, (0, LANES - 2)).reshape(1, LANES)
    own = jnp.concatenate([plane[:own_rows] for plane in planes] + [totals], axis=0)
    spill = jnp.concatenate([plane[own_rows : own_rows + spill_rows] for plane in planes], axis=0)

    mates = [own] + [sent(own, 0, k) for k in range(1, reps)]
    arrivals = [sent(spill, 1, k) for k in range(reps)]
    split = lambda value, rows: tuple(value[rows * i : rows * (i + 1)] for i in range(4))
    merged = functools.reduce(merge, [split(value, own_rows) for value in mates])
    lead = functools.reduce(merge, [split(value, spill_rows) for value in arrivals])
    lead = merge(tuple(part[:spill_rows] for part in merged), lead)
    pen, high, low, gap = (
        jnp.concatenate([head, part[spill_rows:]], axis=0) for head, part in zip(lead, merged)
    )
    empty = pen <= LOWEST_FILL
    key = high.astype(jnp.int32) * 65536 + low.astype(jnp.int32)
    seg_face = jnp.where(empty, -1, FACE_LIMIT - 1 - (key & (FACE_LIMIT - 1)))
    seg_pen = jnp.where(empty, 0.0, pen)

    group = functools.reduce(jnp.add, [value[4 * own_rows :] for value in mates])
    reach = 1
    while reach < doms:
        group = group + sent(group, reach, 0)
        reach *= 2
    mean_gap = group[0, 0] / group[0, 1]
    return (force, seg_pen.reshape(-1), seg_face.reshape(-1), gap.reshape(-1), mean_gap)


def solution(mesh):
    return jax.shard_map(
        shards,
        mesh=mesh,
        in_specs=(
            P(),
            P(),
            P(None, ("dom", "rep")),
            P(None, ("dom", "rep")),
            P(("dom", "rep")),
            P(),
            P(("dom", "rep")),
            P(("dom", "rep")),
            P(("dom", "rep")),
            P(("dom", "rep")),
            P(("dom", "rep")),
        ),
        out_specs=(P(None, ("dom", "rep")), P("dom"), P("dom"), P("dom"), P()),
        check_vma=False,
    )
```

```python
import functools

import jax
import jax.numpy as jnp
from jax import lax
from jax.experimental import pallas as pl
from jax.experimental.pallas import tpu as pltpu
from jax.sharding import PartitionSpec as P

SEG_DEV = 1024
SPILL = 256


PENALTY = 400.0
LOWEST_FILL = -1e30
FACE_LIMIT = 1073741824
LANES = 128
GROUP = 16
NO_KEY = -(2**31)


def pieces_of(value, count):
    parts = []
    for _ in range(count):
        part = value.astype(jnp.bfloat16).astype(jnp.float32)
        parts.append(part)
        value = value - part
    return parts


def local_kernel(
    live_ref,
    ns_ref,
    nm_ref,
    weight_ref,
    sec_ref,
    mst_ref,
    offset_ref,
    jac_ref,
    slot_ref,
    face_ref,
    rank_ref,
    force_ref,
    sent_ref,
    table_w,
    wide_weight,
    table_ref,
):
    step = pl.program_id(0)
    points = ns_ref.shape[1]
    nodes = ns_ref.shape[0]
    rows = sec_ref.shape[1]
    blocks = rows // LANES
    bf16, f32, i32 = jnp.bfloat16, jnp.float32, jnp.int32

    @pl.when(step == 0)
    def _():
        weight = weight_ref[...]
        ns32, nm32 = ns_ref[...].astype(f32), nm_ref[...].astype(f32)
        wide_weight[...] = jnp.transpose(jnp.broadcast_to(weight, (LANES, points)))
        both = jnp.concatenate([ns32, -nm32], axis=0)
        tops = jnp.sum(both * weight, axis=1, keepdims=True)
        ones_at = lax.broadcasted_iota(i32, (GROUP, points), 0) < 3
        total = jnp.sum(weight, axis=1, keepdims=True)
        tails = jnp.broadcast_to(total, (GROUP, LANES))
        tail_parts = pieces_of(tails, 3)
        top_parts = pieces_of(jnp.broadcast_to(tops, (2 * nodes, LANES)), 3)
        lane = lax.broadcasted_iota(i32, (2 * nodes, LANES), 1)
        head = jnp.where(lane == 0, top_parts[0], jnp.where(lane == 1, top_parts[1], jnp.where(lane == 2, top_parts[2], 0.0)))
        lane = lax.broadcasted_iota(i32, (GROUP, LANES), 1)
        sub = lax.broadcasted_iota(i32, (GROUP, LANES), 0)
        foot = jnp.where(lane == 0, tail_parts[0], jnp.where(lane == 1, tail_parts[1], jnp.where(lane == 2, tail_parts[2], 0.0)))
        foot = jnp.where(sub < 3, foot, 0.0)
        left = jnp.concatenate([both, ones_at.astype(f32)], axis=0)
        right = jnp.concatenate([head, foot], axis=0)
        table_w[0:points, :] = jnp.transpose(left).astype(bf16)
        table_w[points:, :] = jnp.transpose(right).astype(bf16)[0:GROUP, :]
        table_ref[0:GROUP, :] = jnp.full((GROUP, LANES), LOWEST_FILL, f32)
        table_ref[GROUP:, :] = jnp.zeros((table_ref.shape[0] - GROUP, LANES), f32)

    live_count = live_ref[0]
    row_ids = (
        step * rows
        + LANES * lax.broadcasted_iota(i32, (blocks, LANES), 0)
        + lax.broadcasted_iota(i32, (blocks, LANES), 1)
    )
    live = row_ids < live_count
    jac = jac_ref[...]

    def as_row(value):
        return jnp.concatenate([value[b : b + 1, :] for b in range(blocks)], axis=1)

    def as_block(value):
        return jnp.concatenate([value[:, LANES * b : LANES * (b + 1)] for b in range(blocks)], axis=0)

    off = pieces_of(offset_ref[...], 3)
    sub = lax.broadcasted_iota(i32, (GROUP, rows), 0)
    off_rows = jnp.where(
        sub == 0, as_row(off[0]), jnp.where(sub == 1, as_row(off[1]), jnp.where(sub == 2, as_row(off[2]), 0.0))
    ).astype(bf16)
    stacked = jnp.concatenate([sec_ref[...], mst_ref[...], off_rows], axis=0)
    gaps = jnp.dot(table_w[...], stacked, preferred_element_type=f32)
    field = gaps[0:points, :]
    pen = as_block(-jnp.min(field, axis=0, keepdims=True))
    weighted = as_block(gaps[points : points + 1, :] + gaps[points + 1 : points + 2, :] + gaps[points + 2 : points + 3, :])

    weights = wide_weight[...]
    scale = jnp.where(live, jac * -PENALTY, 0.0)
    loads = jnp.concatenate(
        [
            (jnp.minimum(field[:, LANES * b : LANES * (b + 1)], 0.0) * weights).astype(bf16)
            for b in range(blocks)
        ],
        axis=1,
    )
    force = jnp.dot(ns_ref[...], loads, preferred_element_type=f32)
    force_ref[...] = (force * as_row(scale)).astype(bf16)

    row_gap = jnp.where(live, jac * weighted, 0.0)
    row_area = jnp.where(live, jac * jnp.sum(weight_ref[...], axis=1, keepdims=True), 0.0)
    table_ref[5 * GROUP : 5 * GROUP + blocks, :] += row_gap
    table_ref[5 * GROUP + 8 : 5 * GROUP + 8 + blocks, :] += row_area

    slot = jnp.where(live, slot_ref[...], (GROUP - 1) * LANES)
    key = ((rank_ref[...] - 2) << 30) + (FACE_LIMIT - 1 - face_ref[...])
    gap_parts = pieces_of(row_gap, 3)
    slot_t, pen_t, key_t = jnp.transpose(slot), jnp.transpose(pen), jnp.transpose(key)
    sub = lax.broadcasted_iota(i32, (LANES, LANES), 0)
    lane = lax.broadcasted_iota(i32, (LANES, LANES), 1)
    group_id = lax.broadcasted_iota(i32, (GROUP, LANES), 0)
    for b in range(blocks):
        slot_col = jnp.broadcast_to(slot_t[:, b : b + 1], (LANES, LANES))
        slot_row = slot[b : b + 1, :]
        same = slot_col == slot_row
        top_pen = jnp.max(jnp.where(same, pen_t[:, b : b + 1], LOWEST_FILL), axis=0, keepdims=True)
        top_key = jnp.max(jnp.where(same, key_t[:, b : b + 1], NO_KEY), axis=0, keepdims=True)
        last = jnp.max(jnp.where(same, sub, -1), axis=0, keepdims=True)
        speaks = last == lax.broadcasted_iota(i32, (1, LANES), 1)
        home = (slot_row >> 7) == group_id
        spoken = home & speaks
        one_hot = jnp.where((slot_col & (LANES - 1)) == lane, 1.0, 0.0).astype(bf16)
        values = pieces_of(top_pen, 3) + [
            (top_key & 255).astype(f32),
            ((top_key >> 8) & 255).astype(f32),
            ((top_key >> 16) & 255).astype(f32),
            (top_key >> 24).astype(f32),
        ]
        picks = [jnp.where(spoken, value, 0.0) for value in values]
        picks.append(jnp.where(spoken, 1.0, 0.0))
        picks += [jnp.where(home, part[b : b + 1, :], 0.0) for part in gap_parts]
        left = jnp.concatenate(picks, axis=0).astype(bf16)
        out = jnp.dot(left, one_hot, preferred_element_type=f32)
        part = [out[GROUP * i : GROUP * (i + 1), :] for i in range(11)]
        there = part[7] > 0.5
        fresh_pen = jnp.where(there, (part[0] + part[1]) + part[2], LOWEST_FILL)
        fresh_high = part[6] * 256.0 + part[5]
        fresh_low = part[4] * 256.0 + part[3]
        old_pen = table_ref[0:GROUP, :]
        old_high = table_ref[GROUP : 2 * GROUP, :]
        old_low = table_ref[2 * GROUP : 3 * GROUP, :]
        fresh_wins = there & (
            (old_pen == LOWEST_FILL)
            | (fresh_high > old_high)
            | ((fresh_high == old_high) & (fresh_low > old_low))
        )
        table_ref[0:GROUP, :] = jnp.maximum(old_pen, fresh_pen)
        table_ref[GROUP : 2 * GROUP, :] = jnp.where(fresh_wins, fresh_high, old_high)
        table_ref[2 * GROUP : 3 * GROUP, :] = jnp.where(fresh_wins, fresh_low, old_low)
        table_ref[3 * GROUP : 4 * GROUP, :] += (part[8] + part[9]) + part[10]

    @pl.when(step == pl.num_programs(0) - 1)
    def _():
        for i in range(PLANES):
            plane = table_ref[GROUP * i : GROUP * (i + 1), :]
            sent_ref[OWN_ROWS * i : OWN_ROWS * (i + 1), :] = plane[:OWN_ROWS]
            at = PLANES * OWN_ROWS + SPILL_ROWS * i
            sent_ref[at : at + SPILL_ROWS, :] = plane[OWN_ROWS : OWN_ROWS + SPILL_ROWS]
        for i in range(2):
            sums = table_ref[5 * GROUP + 8 * i : 5 * GROUP + 8 * (i + 1), :]
            sent_ref[TOTALS_AT + i : TOTALS_AT + i + 1, :] = jnp.sum(sums, axis=0, keepdims=True)
        tail = sent_ref.shape[0] - TOTALS_AT - 2
        sent_ref[TOTALS_AT + 2 :, :] = jnp.zeros((tail, LANES), f32)


def local_step(ns, nm, sec, mst, offset, weight, jac, slot, face, rank, live):
    nodes, points = ns.shape
    row_count = sec.shape[1]
    rows = min(row_count, 1024)
    folded = lambda value: value.reshape(row_count // LANES, LANES)
    whole = lambda shape: pl.BlockSpec(shape, lambda i: (0, 0))
    wide = pl.BlockSpec((nodes, rows), lambda i: (0, i))
    tall = pl.BlockSpec((rows // LANES, LANES), lambda i: (i, 0))
    return pl.pallas_call(
        local_kernel,
        grid=(row_count // rows,),
        in_specs=[
            pl.BlockSpec(memory_space=pltpu.SMEM),
            whole((nodes, points)),
            whole((nodes, points)),
            whole((1, points)),
            wide,
            wide,
            tall,
            tall,
            tall,
            tall,
            tall,
        ],
        out_specs=[wide, whole((SENT_ROWS, LANES))],
        out_shape=[
            jax.ShapeDtypeStruct((nodes, row_count), jnp.bfloat16),
            jax.ShapeDtypeStruct((SENT_ROWS, LANES), jnp.float32),
        ],
        scratch_shapes=[
            pltpu.VMEM((points + GROUP, 2 * nodes + GROUP), jnp.bfloat16),
            pltpu.VMEM((points, LANES), jnp.float32),
            pltpu.VMEM((6 * GROUP, LANES), jnp.float32),
        ],
    )(
        live,
        ns,
        nm,
        weight.reshape(1, points),
        sec,
        mst,
        folded(offset),
        folded(jac),
        folded(slot),
        folded(face),
        folded(rank),
    )


OWN_ROWS = SEG_DEV // LANES
SPILL_ROWS = SPILL // LANES
PLANES = 4
TOTALS_AT = PLANES * (OWN_ROWS + SPILL_ROWS)
SENT_ROWS = -(-(TOTALS_AT + 2) // 8) * 8
PASSED_ROWS = 16


def merge(first, second):
    wins = (second[1] > first[1]) | ((second[1] == first[1]) & (second[2] > first[2]))
    wins = (second[0] > LOWEST_FILL) & (wins | (first[0] <= LOWEST_FILL))
    return (
        jnp.maximum(first[0], second[0]),
        jnp.where(wins, second[1], first[1]),
        jnp.where(wins, second[2], first[2]),
        first[3] + second[3],
    )


def split(value, rows, start=0):
    return tuple(value[start + rows * i : start + rows * (i + 1)] for i in range(PLANES))


def group_kernel(gathered_ref, own_ref, passed_ref):
    parts = [gathered_ref[i] for i in range(gathered_ref.shape[0])]
    own = functools.reduce(merge, [split(part, OWN_ROWS) for part in parts])
    spill_at = PLANES * OWN_ROWS
    spill = functools.reduce(merge, [split(part, SPILL_ROWS, spill_at) for part in parts])
    totals = functools.reduce(jnp.add, [part[TOTALS_AT : TOTALS_AT + 2] for part in parts])
    own_ref[...] = jnp.concatenate(own, axis=0)
    fill = jnp.zeros((PASSED_ROWS - PLANES * SPILL_ROWS - 2, LANES), jnp.float32)
    passed = jnp.concatenate(spill + (totals, fill), axis=0)
    for i in range(passed_ref.shape[0]):
        passed_ref[i] = passed


def final_kernel(before_ref, own_ref, arrived_ref, pen_ref, face_ref, gap_ref, mean_ref):
    own = split(own_ref[...], OWN_ROWS)
    spill = split(arrived_ref[before_ref[0]], SPILL_ROWS)
    lead = merge(tuple(part[:SPILL_ROWS] for part in own), spill)
    pen, high, low, gap = (
        jnp.concatenate([head, part[SPILL_ROWS:]], axis=0) for head, part in zip(lead, own)
    )
    empty = pen <= LOWEST_FILL
    key = high.astype(jnp.int32) * 65536 + low.astype(jnp.int32)
    face_ref[...] = jnp.where(empty, -1, FACE_LIMIT - 1 - (key & (FACE_LIMIT - 1)))
    pen_ref[...] = jnp.where(empty, 0.0, pen)
    gap_ref[...] = gap
    at = PLANES * SPILL_ROWS
    totals = arrived_ref[0, at : at + 2]
    for i in range(1, arrived_ref.shape[0]):
        totals += arrived_ref[i, at : at + 2]
    sums = jnp.sum(totals, axis=1, keepdims=True)
    mean_ref[...] = jnp.broadcast_to(sums[0:1] / sums[1:2], mean_ref.shape)


def shards(ns, nm, sec, mst, offset, weight, jac, slot, face, rank, live):
    doms = lax.axis_size("dom")
    f32 = jnp.float32
    force, table = local_step(ns, nm, sec, mst, offset, weight, jac, slot, face, rank, live)
    gathered = lax.all_gather(table, "rep")
    own, passed = pl.pallas_call(
        group_kernel,
        out_shape=[
            jax.ShapeDtypeStruct((PLANES * OWN_ROWS, LANES), f32),
            jax.ShapeDtypeStruct((doms, PASSED_ROWS, LANES), f32),
        ],
    )(gathered)
    arrived = lax.all_to_all(passed, "dom", 0, 0)
    before = (lax.axis_index("dom") + doms - 1) % doms
    plane = lambda dtype: jax.ShapeDtypeStruct((OWN_ROWS, LANES), dtype)
    vmem = pl.BlockSpec(memory_space=pltpu.VMEM)
    pen, chosen, gap, mean = pl.pallas_call(
        final_kernel,
        in_specs=[pl.BlockSpec(memory_space=pltpu.SMEM), vmem, vmem],
        out_specs=[vmem] * 4,
        out_shape=[plane(f32), plane(jnp.int32), plane(f32), jax.ShapeDtypeStruct((1, 1), f32)],
    )(before.reshape(1), own, arrived)
    return (force, pen.reshape(-1), chosen.reshape(-1), gap.reshape(-1), mean.reshape(()))


def solution(mesh):
    return jax.shard_map(
        shards,
        mesh=mesh,
        in_specs=(
            P(),
            P(),
            P(None, ("dom", "rep")),
            P(None, ("dom", "rep")),
            P(("dom", "rep")),
            P(),
            P(("dom", "rep")),
            P(("dom", "rep")),
            P(("dom", "rep")),
            P(("dom", "rep")),
            P(("dom", "rep")),
        ),
        out_specs=(P(None, ("dom", "rep")), P("dom"), P("dom"), P("dom"), P()),
        check_vma=False,
    )
```

```python
import functools

import jax
import jax.numpy as jnp
from jax import lax
from jax.experimental import pallas as pl
from jax.experimental.pallas import tpu as pltpu
from jax.sharding import PartitionSpec as P

SEG_DEV = 1024
SPILL = 256


PENALTY = 400.0
LOWEST_FILL = -1e30
FACE_LIMIT = 1073741824
LANES = 128
GROUP = 16
NO_KEY = -(2**31)


def pieces_of(value, count):
    parts = []
    for _ in range(count):
        part = value.astype(jnp.bfloat16).astype(jnp.float32)
        parts.append(part)
        value = value - part
    return parts


def as_row(value):
    return jnp.concatenate([value[b : b + 1, :] for b in range(value.shape[0])], axis=1)


def as_block(value):
    return jnp.concatenate(
        [value[:, LANES * b : LANES * (b + 1)] for b in range(value.shape[1] // LANES)], axis=0
    )


def stacked_inputs(sec_ref, mst_ref, offset_ref):
    off = [as_row(part) for part in pieces_of(offset_ref[...], 3)]
    sub = lax.broadcasted_iota(jnp.int32, (GROUP, sec_ref.shape[1]), 0)
    rest = jnp.where(sub == 0, off[0], jnp.where(sub == 1, off[1], jnp.where(sub == 2, off[2], 0.0)))
    return jnp.concatenate([sec_ref[...], mst_ref[...], rest.astype(jnp.bfloat16)], axis=0)


def live_of(shape, live_count):
    row_ids = (
        pl.program_id(0) * (shape[0] * shape[1])
        + shape[1] * lax.broadcasted_iota(jnp.int32, shape, 0)
        + lax.broadcasted_iota(jnp.int32, shape, 1)
    )
    return row_ids < live_count


def force_kernel(
    live_ref, ns_ref, table_ref, weight_ref, sec_ref, mst_ref, offset_ref, jac_ref, force_ref
):
    points = ns_ref.shape[1]
    f32 = jnp.float32
    field = jnp.dot(
        table_ref[0:points, :], stacked_inputs(sec_ref, mst_ref, offset_ref), preferred_element_type=f32
    )
    weights = weight_ref[...]
    loads = [
        (jnp.minimum(field[:, at : at + LANES], 0.0) * weights).astype(jnp.bfloat16)
        for at in range(0, field.shape[1], LANES)
    ]
    force = jnp.dot(ns_ref[...], jnp.concatenate(loads, axis=1), preferred_element_type=f32)
    scale = jnp.where(live_of(jac_ref.shape, live_ref[0]), jac_ref[...] * -PENALTY, 0.0)
    force_ref[...] = (force * as_row(scale)).astype(jnp.bfloat16)


def stats_kernel(
    live_ref,
    ns_ref,
    nm_ref,
    weight_ref,
    sec_ref,
    mst_ref,
    offset_ref,
    jac_ref,
    slot_ref,
    face_ref,
    rank_ref,
    sent_ref,
    table_w,
    wide_weight,
    table_ref,
):
    step = pl.program_id(0)
    points = ns_ref.shape[1]
    nodes = ns_ref.shape[0]
    rows = sec_ref.shape[1]
    blocks = rows // LANES
    bf16, f32, i32 = jnp.bfloat16, jnp.float32, jnp.int32

    @pl.when(step == 0)
    def _():
        weight = weight_ref[...]
        ns32, nm32 = ns_ref[...].astype(f32), nm_ref[...].astype(f32)
        wide_weight[...] = jnp.transpose(jnp.broadcast_to(weight, (LANES, points)))
        both = jnp.concatenate([ns32, -nm32], axis=0)
        tops = jnp.sum(both * weight, axis=1, keepdims=True)
        ones_at = lax.broadcasted_iota(i32, (GROUP, points), 0) < 3
        total = jnp.sum(weight, axis=1, keepdims=True)
        tails = jnp.broadcast_to(total, (GROUP, LANES))
        tail_parts = pieces_of(tails, 3)
        top_parts = pieces_of(jnp.broadcast_to(tops, (2 * nodes, LANES)), 3)
        lane = lax.broadcasted_iota(i32, (2 * nodes, LANES), 1)
        head = jnp.where(lane == 0, top_parts[0], jnp.where(lane == 1, top_parts[1], jnp.where(lane == 2, top_parts[2], 0.0)))
        lane = lax.broadcasted_iota(i32, (GROUP, LANES), 1)
        sub = lax.broadcasted_iota(i32, (GROUP, LANES), 0)
        foot = jnp.where(lane == 0, tail_parts[0], jnp.where(lane == 1, tail_parts[1], jnp.where(lane == 2, tail_parts[2], 0.0)))
        foot = jnp.where(sub < 3, foot, 0.0)
        left = jnp.concatenate([both, ones_at.astype(f32)], axis=0)
        right = jnp.concatenate([head, foot], axis=0)
        table_w[0:points, :] = jnp.transpose(left).astype(bf16)
        table_w[points:, :] = jnp.transpose(right).astype(bf16)[0:GROUP, :]
        table_ref[0:GROUP, :] = jnp.full((GROUP, LANES), LOWEST_FILL, f32)
        table_ref[GROUP:, :] = jnp.zeros((table_ref.shape[0] - GROUP, LANES), f32)

    live = live_of(jac_ref.shape, live_ref[0])
    jac = jac_ref[...]

    gaps = jnp.dot(table_w[...], stacked_inputs(sec_ref, mst_ref, offset_ref), preferred_element_type=f32)
    pen = as_block(-jnp.min(gaps[0:points, :], axis=0, keepdims=True))
    weighted = as_block(
        gaps[points : points + 1, :] + gaps[points + 1 : points + 2, :] + gaps[points + 2 : points + 3, :]
    )

    row_gap = jnp.where(live, jac * weighted, 0.0)
    row_area = jnp.where(live, jac * jnp.sum(weight_ref[...], axis=1, keepdims=True), 0.0)
    table_ref[4 * GROUP : 4 * GROUP + blocks, :] += row_gap
    table_ref[5 * GROUP : 5 * GROUP + blocks, :] += row_area

    slot = jnp.where(live, slot_ref[...], (GROUP - 1) * LANES)
    key = ((rank_ref[...] - 2) << 30) + (FACE_LIMIT - 1 - face_ref[...])
    gap_parts = pieces_of(row_gap, 3)
    slot_t, pen_t, key_t = jnp.transpose(slot), jnp.transpose(pen), jnp.transpose(key)
    place = lax.broadcasted_iota(i32, (LANES, LANES), 0).astype(f32)
    lane = lax.broadcasted_iota(i32, (LANES, LANES), 1)
    group_id = lax.broadcasted_iota(i32, (GROUP, LANES), 0)
    old_pen, old_high, old_low, old_gap = (table_ref[GROUP * i : GROUP * (i + 1), :] for i in range(PLANES))
    for b in range(blocks):
        slot_col = jnp.broadcast_to(slot_t[:, b : b + 1], (LANES, LANES))
        slot_row = slot[b : b + 1, :]
        same = slot_col == slot_row
        top_pen = jnp.max(jnp.where(same, pen_t[:, b : b + 1], LOWEST_FILL), axis=0, keepdims=True)
        top_key = jnp.max(jnp.where(same, key_t[:, b : b + 1], NO_KEY), axis=0, keepdims=True)
        last = jnp.max(jnp.where(same, place, -1.0), axis=0, keepdims=True)
        speaks = last == lax.broadcasted_iota(i32, (1, LANES), 1).astype(f32)
        home = (slot_row >> 7) == group_id
        spoken = home & speaks
        one_hot = jnp.where((slot_col & (LANES - 1)) == lane, 1.0, 0.0).astype(bf16)
        values = pieces_of(top_pen, 3) + [
            (top_key & 255).astype(f32),
            ((top_key >> 8) & 255).astype(f32),
            ((top_key >> 16) & 255).astype(f32),
            (top_key >> 24).astype(f32),
        ]
        picks = [jnp.where(spoken, value, 0.0) for value in values]
        picks.append(jnp.where(spoken, 1.0, 0.0))
        picks += [jnp.where(home, part[b : b + 1, :], 0.0) for part in gap_parts]
        left = jnp.concatenate(picks, axis=0).astype(bf16)
        out = jnp.dot(left, one_hot, preferred_element_type=f32)
        part = [out[GROUP * i : GROUP * (i + 1), :] for i in range(11)]
        there = part[7] > 0.5
        fresh_pen = jnp.where(there, (part[0] + part[1]) + part[2], LOWEST_FILL)
        fresh_high = part[6] * 256.0 + part[5]
        fresh_low = part[4] * 256.0 + part[3]
        fresh_wins = there & (
            (old_pen == LOWEST_FILL)
            | (fresh_high > old_high)
            | ((fresh_high == old_high) & (fresh_low > old_low))
        )
        old_pen = jnp.maximum(old_pen, fresh_pen)
        old_high = jnp.where(fresh_wins, fresh_high, old_high)
        old_low = jnp.where(fresh_wins, fresh_low, old_low)
        old_gap += (part[8] + part[9]) + part[10]
    for i, plane in enumerate((old_pen, old_high, old_low, old_gap)):
        table_ref[GROUP * i : GROUP * (i + 1), :] = plane

    @pl.when(step == pl.num_programs(0) - 1)
    def _():
        for i in range(PLANES):
            plane = table_ref[GROUP * i : GROUP * (i + 1), :]
            sent_ref[OWN_ROWS * i : OWN_ROWS * (i + 1), :] = plane[:OWN_ROWS]
            at = PLANES * OWN_ROWS + SPILL_ROWS * i
            sent_ref[at : at + SPILL_ROWS, :] = plane[OWN_ROWS : OWN_ROWS + SPILL_ROWS]
        for i in range(2):
            sums = table_ref[(PLANES + i) * GROUP : (PLANES + i + 1) * GROUP, :]
            sent_ref[TOTALS_AT + i : TOTALS_AT + i + 1, :] = jnp.sum(sums, axis=0, keepdims=True)
        tail = sent_ref.shape[0] - TOTALS_AT - 2
        sent_ref[TOTALS_AT + 2 :, :] = jnp.zeros((tail, LANES), f32)


def specs_of(ns, sec):
    nodes, row_count = ns.shape[0], sec.shape[1]
    rows = min(row_count, GROUP * LANES)
    wide = pl.BlockSpec((nodes, rows), lambda i: (0, i))
    tall = pl.BlockSpec((rows // LANES, LANES), lambda i: (i, 0))
    return (row_count // rows,), wide, tall


def whole(shape):
    return pl.BlockSpec(shape, lambda i: (0, 0))


def stats_of(ns, nm, sec, mst, offset, weight, jac, slot, face, rank, live):
    nodes, points = ns.shape
    grid, wide, tall = specs_of(ns, sec)
    shapes = [
        ((SENT_ROWS, LANES), jnp.float32),
        ((points + GROUP, 2 * nodes + GROUP), jnp.bfloat16),
        ((points, LANES), jnp.float32),
    ]
    return pl.pallas_call(
        stats_kernel,
        grid=grid,
        in_specs=[pl.BlockSpec(memory_space=pltpu.SMEM)]
        + [whole(ns.shape)] * 2
        + [whole((1, points))]
        + [wide] * 2
        + [tall] * 5,
        out_specs=[whole(shape) for shape, _ in shapes],
        out_shape=[jax.ShapeDtypeStruct(shape, dtype) for shape, dtype in shapes],
        scratch_shapes=[pltpu.VMEM((6 * GROUP, LANES), jnp.float32)],
    )(live, ns, nm, weight.reshape(1, points), sec, mst, offset, jac, slot, face, rank)


def force_of(ns, table, weight, sec, mst, offset, jac, live):
    grid, wide, tall = specs_of(ns, sec)
    nodes, points = ns.shape
    work = 2 * sec.shape[1] * points * (3 * nodes + GROUP)
    return pl.pallas_call(
        force_kernel,
        grid=grid,
        in_specs=[pl.BlockSpec(memory_space=pltpu.SMEM)]
        + [whole(ns.shape), whole(table.shape), whole(weight.shape)]
        + [wide] * 2
        + [tall] * 2,
        out_specs=wide,
        out_shape=jax.ShapeDtypeStruct(sec.shape, jnp.bfloat16),
        cost_estimate=pl.CostEstimate(flops=20 * work, bytes_accessed=6 * sec.size, transcendentals=0),
    )(live, ns, table, weight, sec, mst, offset, jac)


OWN_ROWS = SEG_DEV // LANES
SPILL_ROWS = SPILL // LANES
PLANES = 4
TOTALS_AT = PLANES * (OWN_ROWS + SPILL_ROWS)
SENT_ROWS = -(-(TOTALS_AT + 2) // 8) * 8
PASSED_ROWS = 16


def merge(first, second):
    wins = (second[1] > first[1]) | ((second[1] == first[1]) & (second[2] > first[2]))
    wins = (second[0] > LOWEST_FILL) & (wins | (first[0] <= LOWEST_FILL))
    return (
        jnp.maximum(first[0], second[0]),
        jnp.where(wins, second[1], first[1]),
        jnp.where(wins, second[2], first[2]),
        first[3] + second[3],
    )


def split(value, rows, start=0):
    return tuple(value[start + rows * i : start + rows * (i + 1)] for i in range(PLANES))


def group_kernel(gathered_ref, own_ref, passed_ref):
    parts = [gathered_ref[i] for i in range(gathered_ref.shape[0])]
    own = functools.reduce(merge, [split(part, OWN_ROWS) for part in parts])
    spill_at = PLANES * OWN_ROWS
    spill = functools.reduce(merge, [split(part, SPILL_ROWS, spill_at) for part in parts])
    totals = functools.reduce(jnp.add, [part[TOTALS_AT : TOTALS_AT + 2] for part in parts])
    own_ref[...] = jnp.concatenate(own, axis=0)
    fill = jnp.zeros((PASSED_ROWS - PLANES * SPILL_ROWS - 2, LANES), jnp.float32)
    passed = jnp.concatenate(spill + (totals, fill), axis=0)
    for i in range(passed_ref.shape[0]):
        passed_ref[i] = passed


def final_kernel(before_ref, own_ref, arrived_ref, pen_ref, face_ref, gap_ref, mean_ref):
    own = split(own_ref[...], OWN_ROWS)
    spill = split(arrived_ref[before_ref[0]], SPILL_ROWS)
    lead = merge(tuple(part[:SPILL_ROWS] for part in own), spill)
    pen, high, low, gap = (
        jnp.concatenate([head, part[SPILL_ROWS:]], axis=0) for head, part in zip(lead, own)
    )
    empty = pen <= LOWEST_FILL
    key = high.astype(jnp.int32) * 65536 + low.astype(jnp.int32)
    face_ref[...] = jnp.where(empty, -1, FACE_LIMIT - 1 - (key & (FACE_LIMIT - 1)))
    pen_ref[...] = jnp.where(empty, 0.0, pen)
    gap_ref[...] = gap
    at = PLANES * SPILL_ROWS
    totals = arrived_ref[0, at : at + 2]
    for i in range(1, arrived_ref.shape[0]):
        totals += arrived_ref[i, at : at + 2]
    sums = jnp.sum(totals, axis=1, keepdims=True)
    mean_ref[...] = jnp.broadcast_to(sums[0:1] / sums[1:2], mean_ref.shape)


def shards(ns, nm, sec, mst, offset, weight, jac, slot, face, rank, live):
    doms = lax.axis_size("dom")
    f32 = jnp.float32
    offset, jac, slot, face, rank = (
        value.reshape(-1, LANES) for value in (offset, jac, slot, face, rank)
    )
    table, table_w, wide_weight = stats_of(
        ns, nm, sec, mst, offset, weight, jac, slot, face, rank, live
    )
    gathered = lax.all_gather(table, "rep")
    own, passed = pl.pallas_call(
        group_kernel,
        out_shape=[
            jax.ShapeDtypeStruct((PLANES * OWN_ROWS, LANES), f32),
            jax.ShapeDtypeStruct((doms, PASSED_ROWS, LANES), f32),
        ],
    )(gathered)
    arrived = lax.all_to_all(passed, "dom", 0, 0)
    force = force_of(ns, table_w, wide_weight, sec, mst, offset, jac, live)
    before = (lax.axis_index("dom") + doms - 1) % doms
    plane = lambda dtype: jax.ShapeDtypeStruct((OWN_ROWS, LANES), dtype)
    vmem = pl.BlockSpec(memory_space=pltpu.VMEM)
    pen, chosen, gap, mean = pl.pallas_call(
        final_kernel,
        in_specs=[pl.BlockSpec(memory_space=pltpu.SMEM), vmem, vmem],
        out_specs=[vmem] * 4,
        out_shape=[plane(f32), plane(jnp.int32), plane(f32), jax.ShapeDtypeStruct((1, 1), f32)],
    )(before.reshape(1), own, arrived)
    return (force, pen.reshape(-1), chosen.reshape(-1), gap.reshape(-1), mean.reshape(()))


def solution(mesh):
    return jax.shard_map(
        shards,
        mesh=mesh,
        in_specs=(
            P(),
            P(),
            P(None, ("dom", "rep")),
            P(None, ("dom", "rep")),
            P(("dom", "rep")),
            P(),
            P(("dom", "rep")),
            P(("dom", "rep")),
            P(("dom", "rep")),
            P(("dom", "rep")),
            P(("dom", "rep")),
        ),
        out_specs=(P(None, ("dom", "rep")), P("dom"), P("dom"), P("dom"), P()),
        check_vma=False,
    )
```

```python
import functools

import jax
import jax.numpy as jnp
from jax import lax
from jax.experimental import pallas as pl
from jax.experimental.pallas import tpu as pltpu
from jax.sharding import PartitionSpec as P

SEG_DEV = 1024
SPILL = 256


PENALTY = 400.0
LOWEST_FILL = -1e30
FACE_LIMIT = 1073741824
LANES = 128
GROUP = 16
NO_KEY = -(2**31)


def pieces_of(value, count):
    parts = []
    for _ in range(count):
        part = value.astype(jnp.bfloat16).astype(jnp.float32)
        parts.append(part)
        value = value - part
    return parts


def as_row(value):
    return jnp.concatenate([value[b : b + 1, :] for b in range(value.shape[0])], axis=1)


def as_block(value):
    return jnp.concatenate(
        [value[:, LANES * b : LANES * (b + 1)] for b in range(value.shape[1] // LANES)], axis=0
    )


def stacked_inputs(sec_ref, mst_ref, offset_ref):
    off = [as_row(part) for part in pieces_of(offset_ref[...], 3)]
    sub = lax.broadcasted_iota(jnp.int32, (GROUP, sec_ref.shape[1]), 0)
    rest = jnp.where(sub == 0, off[0], jnp.where(sub == 1, off[1], jnp.where(sub == 2, off[2], 0.0)))
    return jnp.concatenate([sec_ref[...], mst_ref[...], rest.astype(jnp.bfloat16)], axis=0)


def live_of(shape, live_count):
    row_ids = (
        pl.program_id(0) * (shape[0] * shape[1])
        + shape[1] * lax.broadcasted_iota(jnp.int32, shape, 0)
        + lax.broadcasted_iota(jnp.int32, shape, 1)
    )
    return row_ids < live_count


def force_kernel(
    live_ref, ns_ref, table_ref, weight_ref, sec_ref, mst_ref, offset_ref, jac_ref, force_ref
):
    points = ns_ref.shape[1]
    f32 = jnp.float32
    field = jnp.dot(
        table_ref[0:points, :], stacked_inputs(sec_ref, mst_ref, offset_ref), preferred_element_type=f32
    )
    weights = weight_ref[...]
    loads = [
        (jnp.minimum(field[:, at : at + LANES], 0.0) * weights).astype(jnp.bfloat16)
        for at in range(0, field.shape[1], LANES)
    ]
    force = jnp.dot(ns_ref[...], jnp.concatenate(loads, axis=1), preferred_element_type=f32)
    scale = jnp.where(live_of(jac_ref.shape, live_ref[0]), jac_ref[...] * -PENALTY, 0.0)
    force_ref[...] = (force * as_row(scale)).astype(jnp.bfloat16)


def stats_kernel(
    live_ref,
    ns_ref,
    nm_ref,
    weight_ref,
    sec_ref,
    mst_ref,
    offset_ref,
    jac_ref,
    slot_ref,
    face_ref,
    rank_ref,
    sent_ref,
    table_w,
    wide_weight,
    table_ref,
):
    step = pl.program_id(0)
    points = ns_ref.shape[1]
    nodes = ns_ref.shape[0]
    rows = sec_ref.shape[1]
    blocks = rows // LANES
    bf16, f32, i32 = jnp.bfloat16, jnp.float32, jnp.int32

    @pl.when(step == 0)
    def _():
        weight = weight_ref[...]
        ns32, nm32 = ns_ref[...].astype(f32), nm_ref[...].astype(f32)
        wide_weight[...] = jnp.transpose(jnp.broadcast_to(weight, (LANES, points)))
        both = jnp.concatenate([ns32, -nm32], axis=0)
        tops = jnp.sum(both * weight, axis=1, keepdims=True)
        ones_at = lax.broadcasted_iota(i32, (GROUP, points), 0) < 3
        total = jnp.sum(weight, axis=1, keepdims=True)
        tails = jnp.broadcast_to(total, (GROUP, LANES))
        tail_parts = pieces_of(tails, 3)
        top_parts = pieces_of(jnp.broadcast_to(tops, (2 * nodes, LANES)), 3)
        lane = lax.broadcasted_iota(i32, (2 * nodes, LANES), 1)
        head = jnp.where(lane == 0, top_parts[0], jnp.where(lane == 1, top_parts[1], jnp.where(lane == 2, top_parts[2], 0.0)))
        lane = lax.broadcasted_iota(i32, (GROUP, LANES), 1)
        sub = lax.broadcasted_iota(i32, (GROUP, LANES), 0)
        foot = jnp.where(lane == 0, tail_parts[0], jnp.where(lane == 1, tail_parts[1], jnp.where(lane == 2, tail_parts[2], 0.0)))
        foot = jnp.where(sub < 3, foot, 0.0)
        left = jnp.concatenate([both, ones_at.astype(f32)], axis=0)
        right = jnp.concatenate([head, foot], axis=0)
        table_w[0:points, :] = jnp.transpose(left).astype(bf16)
        table_w[points:, :] = jnp.transpose(right).astype(bf16)[0:GROUP, :]
        table_ref[0:GROUP, :] = jnp.full((GROUP, LANES), LOWEST_FILL, f32)
        table_ref[GROUP:, :] = jnp.zeros((table_ref.shape[0] - GROUP, LANES), f32)

    live = live_of(jac_ref.shape, live_ref[0])
    jac = jac_ref[...]

    gaps = jnp.dot(table_w[...], stacked_inputs(sec_ref, mst_ref, offset_ref), preferred_element_type=f32)
    pen = as_block(-jnp.min(gaps[0:points, :], axis=0, keepdims=True))
    weighted = as_block(
        gaps[points : points + 1, :] + gaps[points + 1 : points + 2, :] + gaps[points + 2 : points + 3, :]
    )

    row_gap = jnp.where(live, jac * weighted, 0.0)
    row_area = jnp.where(live, jac * jnp.sum(weight_ref[...], axis=1, keepdims=True), 0.0)
    table_ref[4 * GROUP : 4 * GROUP + blocks, :] += row_gap
    table_ref[5 * GROUP : 5 * GROUP + blocks, :] += row_area

    slot = jnp.where(live, slot_ref[...], (GROUP - 1) * LANES)
    key = ((rank_ref[...] - 2) << 30) + (FACE_LIMIT - 1 - face_ref[...])
    gap_parts = pieces_of(row_gap, 3)
    slot_t, pen_t, key_t = jnp.transpose(slot), jnp.transpose(pen), jnp.transpose(key)
    place = lax.broadcasted_iota(i32, (LANES, LANES), 0).astype(f32)
    lane = lax.broadcasted_iota(i32, (LANES, LANES), 1)
    group_id = lax.broadcasted_iota(i32, (GROUP, LANES), 0)
    old_pen, old_high, old_low, old_gap = (table_ref[GROUP * i : GROUP * (i + 1), :] for i in range(PLANES))
    for b in range(blocks):
        slot_col = jnp.broadcast_to(slot_t[:, b : b + 1], (LANES, LANES))
        slot_row = slot[b : b + 1, :]
        same = slot_col == slot_row
        top_pen = jnp.max(jnp.where(same, pen_t[:, b : b + 1], LOWEST_FILL), axis=0, keepdims=True)
        top_key = jnp.max(jnp.where(same, key_t[:, b : b + 1], NO_KEY), axis=0, keepdims=True)
        last = jnp.max(jnp.where(same, place, -1.0), axis=0, keepdims=True)
        speaks = last == lax.broadcasted_iota(i32, (1, LANES), 1).astype(f32)
        home = (slot_row >> 7) == group_id
        spoken = home & speaks
        one_hot = jnp.where((slot_col & (LANES - 1)) == lane, 1.0, 0.0).astype(bf16)
        values = pieces_of(top_pen, 3) + [
            (top_key & 255).astype(f32),
            ((top_key >> 8) & 255).astype(f32),
            ((top_key >> 16) & 255).astype(f32),
            (top_key >> 24).astype(f32),
        ]
        picks = [jnp.where(spoken, value, 0.0) for value in values]
        picks.append(jnp.where(spoken, 1.0, 0.0))
        picks += [jnp.where(home, part[b : b + 1, :], 0.0) for part in gap_parts]
        left = jnp.concatenate(picks, axis=0).astype(bf16)
        out = jnp.dot(left, one_hot, preferred_element_type=f32)
        part = [out[GROUP * i : GROUP * (i + 1), :] for i in range(11)]
        there = part[7] > 0.5
        fresh_pen = jnp.where(there, (part[0] + part[1]) + part[2], LOWEST_FILL)
        fresh_high = part[6] * 256.0 + part[5]
        fresh_low = part[4] * 256.0 + part[3]
        fresh_wins = there & (
            (old_pen == LOWEST_FILL)
            | (fresh_high > old_high)
            | ((fresh_high == old_high) & (fresh_low > old_low))
        )
        old_pen = jnp.maximum(old_pen, fresh_pen)
        old_high = jnp.where(fresh_wins, fresh_high, old_high)
        old_low = jnp.where(fresh_wins, fresh_low, old_low)
        old_gap += (part[8] + part[9]) + part[10]
    for i, plane in enumerate((old_pen, old_high, old_low, old_gap)):
        table_ref[GROUP * i : GROUP * (i + 1), :] = plane

    @pl.when(step == pl.num_programs(0) - 1)
    def _():
        for i in range(PLANES):
            plane = table_ref[GROUP * i : GROUP * (i + 1), :]
            sent_ref[OWN_ROWS * i : OWN_ROWS * (i + 1), :] = plane[:OWN_ROWS]
            at = PLANES * OWN_ROWS + SPILL_ROWS * i
            sent_ref[at : at + SPILL_ROWS, :] = plane[OWN_ROWS : OWN_ROWS + SPILL_ROWS]
        for i in range(2):
            sums = table_ref[(PLANES + i) * GROUP : (PLANES + i + 1) * GROUP, :]
            sent_ref[TOTALS_AT + i : TOTALS_AT + i + 1, :] = jnp.sum(sums, axis=0, keepdims=True)
        tail = sent_ref.shape[0] - TOTALS_AT - 2
        sent_ref[TOTALS_AT + 2 :, :] = jnp.zeros((tail, LANES), f32)


def specs_of(ns, sec):
    nodes, row_count = ns.shape[0], sec.shape[1]
    rows = min(row_count, GROUP * LANES)
    wide = pl.BlockSpec((nodes, rows), lambda i: (0, i))
    tall = pl.BlockSpec((rows // LANES, LANES), lambda i: (i, 0))
    return (row_count // rows,), wide, tall


def whole(shape):
    return pl.BlockSpec(shape, lambda i: (0, 0))


def stats_of(ns, nm, sec, mst, offset, weight, jac, slot, face, rank, live):
    nodes, points = ns.shape
    grid, wide, tall = specs_of(ns, sec)
    shapes = [
        ((SENT_ROWS, LANES), jnp.float32),
        ((points + GROUP, 2 * nodes + GROUP), jnp.bfloat16),
        ((points, LANES), jnp.float32),
    ]
    return pl.pallas_call(
        stats_kernel,
        grid=grid,
        in_specs=[pl.BlockSpec(memory_space=pltpu.SMEM)]
        + [whole(ns.shape)] * 2
        + [whole((1, points))]
        + [wide] * 2
        + [tall] * 5,
        out_specs=[whole(shape) for shape, _ in shapes],
        out_shape=[jax.ShapeDtypeStruct(shape, dtype) for shape, dtype in shapes],
        scratch_shapes=[pltpu.VMEM((6 * GROUP, LANES), jnp.float32)],
    )(live, ns, nm, weight.reshape(1, points), sec, mst, offset, jac, slot, face, rank)


def force_of(ns, table, weight, sec, mst, offset, jac, live):
    grid, wide, tall = specs_of(ns, sec)
    nodes, points = ns.shape
    work = 2 * sec.shape[1] * points * (3 * nodes + GROUP)
    return pl.pallas_call(
        force_kernel,
        grid=grid,
        in_specs=[pl.BlockSpec(memory_space=pltpu.SMEM)]
        + [whole(ns.shape), whole(table.shape), whole(weight.shape)]
        + [wide] * 2
        + [tall] * 2,
        out_specs=wide,
        out_shape=jax.ShapeDtypeStruct(sec.shape, jnp.bfloat16),
        cost_estimate=pl.CostEstimate(flops=20 * work, bytes_accessed=6 * sec.size, transcendentals=0),
    )(live, ns, table, weight, sec, mst, offset, jac)


OWN_ROWS = SEG_DEV // LANES
SPILL_ROWS = SPILL // LANES
PLANES = 4
TOTALS_AT = PLANES * (OWN_ROWS + SPILL_ROWS)
SENT_ROWS = -(-(TOTALS_AT + 2) // 8) * 8
PASSED_ROWS = 16


def merge(first, second):
    wins = (second[1] > first[1]) | ((second[1] == first[1]) & (second[2] > first[2]))
    wins = (second[0] > LOWEST_FILL) & (wins | (first[0] <= LOWEST_FILL))
    return (
        jnp.maximum(first[0], second[0]),
        jnp.where(wins, second[1], first[1]),
        jnp.where(wins, second[2], first[2]),
        first[3] + second[3],
    )


def split(value, rows, start=0):
    return tuple(value[start + rows * i : start + rows * (i + 1)] for i in range(PLANES))


def in_pairs(join, parts):
    while len(parts) > 1 and len(parts) % 2 == 0:
        half = len(parts) // 2
        parts = [join(parts[i], parts[i + half]) for i in range(half)]
    return functools.reduce(join, parts)


def group_kernel(*refs):
    own_ref, passed_ref = refs[-2:]
    parts = [ref[...] for ref in refs[:-2]]
    own = in_pairs(merge, [split(part, OWN_ROWS) for part in parts])
    spill_at = PLANES * OWN_ROWS
    spill = in_pairs(merge, [split(part, SPILL_ROWS, spill_at) for part in parts])
    totals = in_pairs(jnp.add, [part[TOTALS_AT : TOTALS_AT + 2] for part in parts])
    own_ref[...] = jnp.concatenate(own, axis=0)
    fill = jnp.zeros((PASSED_ROWS - PLANES * SPILL_ROWS - 2, LANES), jnp.float32)
    passed = jnp.concatenate(spill + (totals, fill), axis=0)
    for i in range(passed_ref.shape[0]):
        passed_ref[i] = passed


def final_kernel(before_ref, own_ref, arrived_ref, pen_ref, face_ref, gap_ref, mean_ref):
    own = split(own_ref[...], OWN_ROWS)
    spill = split(arrived_ref[before_ref[0]], SPILL_ROWS)
    lead = merge(tuple(part[:SPILL_ROWS] for part in own), spill)
    pen, high, low, gap = (
        jnp.concatenate([head, part[SPILL_ROWS:]], axis=0) for head, part in zip(lead, own)
    )
    empty = pen <= LOWEST_FILL
    key = high.astype(jnp.int32) * 65536 + low.astype(jnp.int32)
    face_ref[...] = jnp.where(empty, -1, FACE_LIMIT - 1 - (key & (FACE_LIMIT - 1)))
    pen_ref[...] = jnp.where(empty, 0.0, pen)
    gap_ref[...] = gap
    at = PLANES * SPILL_ROWS
    totals = arrived_ref[0, at : at + 2]
    for i in range(1, arrived_ref.shape[0]):
        totals += arrived_ref[i, at : at + 2]
    sums = jnp.sum(totals, axis=1, keepdims=True)
    mean_ref[...] = jnp.broadcast_to(sums[0:1] / sums[1:2], mean_ref.shape)


def shards(ns, nm, sec, mst, offset, weight, jac, slot, face, rank, live):
    doms = lax.axis_size("dom")
    f32 = jnp.float32
    offset, jac, slot, face, rank = (
        value.reshape(-1, LANES) for value in (offset, jac, slot, face, rank)
    )
    table, table_w, wide_weight = stats_of(
        ns, nm, sec, mst, offset, weight, jac, slot, face, rank, live
    )
    reps = lax.axis_size("rep")
    mates = [table] + [
        lax.ppermute(table, "rep", [(i, (i + k) % reps) for i in range(reps)]) for k in range(1, reps)
    ]
    own, passed = pl.pallas_call(
        group_kernel,
        out_shape=[
            jax.ShapeDtypeStruct((PLANES * OWN_ROWS, LANES), f32),
            jax.ShapeDtypeStruct((doms, PASSED_ROWS, LANES), f32),
        ],
    )(*mates)
    arrived = lax.all_to_all(passed, "dom", 0, 0)
    force = force_of(ns, table_w, wide_weight, sec, mst, offset, jac, live)
    before = (lax.axis_index("dom") + doms - 1) % doms
    plane = lambda dtype: jax.ShapeDtypeStruct((OWN_ROWS, LANES), dtype)
    vmem = pl.BlockSpec(memory_space=pltpu.VMEM)
    pen, chosen, gap, mean = pl.pallas_call(
        final_kernel,
        in_specs=[pl.BlockSpec(memory_space=pltpu.SMEM), vmem, vmem],
        out_specs=[vmem] * 4,
        out_shape=[plane(f32), plane(jnp.int32), plane(f32), jax.ShapeDtypeStruct((1, 1), f32)],
    )(before.reshape(1), own, arrived)
    return (force, pen.reshape(-1), chosen.reshape(-1), gap.reshape(-1), mean.reshape(()))


def solution(mesh):
    return jax.shard_map(
        shards,
        mesh=mesh,
        in_specs=(
            P(),
            P(),
            P(None, ("dom", "rep")),
            P(None, ("dom", "rep")),
            P(("dom", "rep")),
            P(),
            P(("dom", "rep")),
            P(("dom", "rep")),
            P(("dom", "rep")),
            P(("dom", "rep")),
            P(("dom", "rep")),
        ),
        out_specs=(P(None, ("dom", "rep")), P("dom"), P("dom"), P("dom"), P()),
        check_vma=False,
    )
```
